32 devices in a mesh: expert: 16 (over z, y, core), tensor: 2 (over x).
Axes of the slice: x: 2, y: 2, z: 4, core: 2. Of those that a mesh axis runs over, the one named last changes fastest.
Arguments:
- tokens: bfloat16 [4096, 2560], P(('expert', 'tensor')), may hold values from -6 to 6
- expert_ids: int32 [4096, 1], P(('expert', 'tensor')), may hold values from 0 to 7; in each aligned block of 128 rows (0 to 127, 128 to 255, ...) at most 24 rows name the same one
- gate_weights: bfloat16 [4096, 1], P(('expert', 'tensor')), may hold values from 0.19921875 to 1
- routed_up: bfloat16 [16, 2560, 2048], P('expert', None, 'tensor'), may hold values from -0.125 to 0.125
- routed_down: bfloat16 [16, 2048, 2560], P('expert', 'tensor'), may hold values from -0.09375 to 0.09375
- shared_up: bfloat16 [2560, 4096], P('expert', 'tensor'), may hold values from -0.125 to 0.125
- shared_down: bfloat16 [4096, 2560], P('tensor', 'expert'), may hold values from -0.09375 to 0.09375
Outputs:
- layer_out: bfloat16 [4096, 2560], P(('expert', 'tensor'))
The draws below stay inside these ranges and needn't reach their ends.
Inputs may be any that keep to these rules, and one draw needn't show every extreme that they name: `expert_ids`: each token names one of 8 experts; among the 128 tokens of one device at most 24 name the same expert, and in every draw some device's tokens name one expert exactly 24 times.
All inputs are finite; a program needn't handle non-finite values.
Results may differ from the reference program's by a relative error of at most 0.0073.
Values may be sent and summed in bfloat16 or wider, within the bound.
A program may use at most 128 MiB of HBM per device.

```python
import math
import jax
import jax.numpy as jnp
import numpy as np
from jax import lax

D = 2560
H_WIN = 4096
SH = 4096
TOK_DEV = 128
EXPERTS = 8
CAP = 24
TOKENS = 4096
N_TENSOR = 2


def steps_of(rng, dims, shards, least, largest):
    def one(dim, blocks):
        heights = jax.random.uniform(jax.random.fold_in(jax.random.fold_in(rng, 6), dim), (blocks,), jnp.float32, least / len(shards), largest / len(shards))
        return jnp.repeat(jnp.exp(heights), dims[dim] // blocks).reshape((-1,) + (1,) * (len(dims) - dim - 1))

    level = one(*shards[0])
    for cut in shards[1:]:
        level = level * one(*cut)
    return level


def deal_out(key, own, number, rows, amount, top, most, slope):
    sequence = jax.random.permutation(key, amount)
    crowded, ordinary = portions_of(amount, rows * top, most, slope, True), portions_of(amount, rows * top, most, slope, False)
    places = jnp.arange(amount)

    def named(tallies, rotation):
        used = int((tallies > 0).sum())
        fixed = max(1, used // 4)
        shifted = fixed + (places - fixed + rotation * (used - fixed)) % max(1, amount - fixed)
        return jnp.zeros((amount,), jnp.int32).at[sequence[jnp.where(places < fixed, places, shifted)]].set(jnp.asarray(tallies, jnp.int32))

    tallies = jnp.where(number % 4 == 0, named(crowded, number // 4), named(ordinary, number - number // 4 - 1))
    mixed = jax.random.permutation(jax.random.fold_in(own, 3), amount)
    source_of, receiver = mixed[0:amount // 2 * 2:2], mixed[1:amount // 2 * 2:2]
    room = jnp.minimum(tallies[source_of] - 1, most - tallies[receiver]) // 2
    room = jnp.where((source_of == sequence[0]) | (receiver == sequence[0]) | (tallies[receiver] == 0), 0, jnp.maximum(room, 0))
    shifted = jax.random.randint(jax.random.fold_in(own, 4), (amount // 2,), 0, 1 << 20) % (room + 1)
    tallies = tallies.at[source_of].add(-shifted).at[receiver].add(shifted)
    items = jnp.searchsorted(jnp.cumsum(tallies), jnp.arange(rows * top), side="right").astype(jnp.int32)
    table = items.reshape(top, rows).T
    table = table[jax.random.permutation(jax.random.fold_in(own, 1), rows)]
    rotation = jax.random.randint(jax.random.fold_in(own, 2), (rows, 1), 0, top)
    return jnp.take_along_axis(table, (jnp.arange(top)[None, :] + rotation) % top, axis=1)


def portions_of(count, total, most, skew, full):
    portions = [(1 << 20) // math.isqrt(standing ** skew) + 1 for standing in range(1, count + 1)]
    largest = most if full else min(most, max(-(-total // count), total * portions[0] // sum(portions)))
    least = 1 if total - largest >= count - 1 else 0
    given, rest = [largest] + [least] * (count - 1), total - largest - least * (count - 1)
    while rest > 0:
        movable = [i for i in range(1, count) if given[i] < largest] or [i for i in range(1, count) if given[i] < most]
        pool, left = sum([portions[i] for i in movable]), rest
        for i in movable:
            extra = min(most - given[i], max(1, left * portions[i] // pool), rest)
            given[i] = given[i] + extra
            rest = rest - extra
    return np.array(given)


def bell_draw(key, dims, width, limit, split=(), kind=jnp.bfloat16):
    entries = width * jax.random.normal(key, dims, jnp.float32)
    if split:
        entries = entries * steps_of(key, dims, split, -0.22, 0.18)
    return jnp.clip(entries, -limit, limit).astype(kind)


def setup_inputs(seed: int = 0) -> dict:
    key_of = jax.random.split(jax.random.key(seed), 8)
    tokens = bell_draw(key_of[0], (TOKENS, D), 1.0, 6.0, ((0, 32),))
    expert_ids_keys = jax.random.split(jax.random.fold_in(key_of[1], 1), TOKENS // TOK_DEV)
    expert_ids_turns = jax.random.permutation(jax.random.fold_in(key_of[1], 3), TOKENS // TOK_DEV)
    expert_ids = jax.vmap(lambda own, number: deal_out(jax.random.fold_in(key_of[1], 2), own, number, TOK_DEV, EXPERTS, 1, CAP, 2))(expert_ids_keys, expert_ids_turns).reshape((TOKENS, 1))
    gate_weights = jnp.clip(0.19921875 + 0.80078125 * jax.random.uniform(key_of[2], (TOKENS, 1), jnp.float32) ** steps_of(key_of[2], (TOKENS, 1), ((0, 32),), -0.2, 0.2), 0.19921875, 1.0).astype(jnp.bfloat16)
    routed_up = bell_draw(key_of[3], (2 * EXPERTS, D, H_WIN // 2), D ** -0.5, 0.125, ((0, 16), (2, 2)))
    routed_down = bell_draw(key_of[4], (2 * EXPERTS, H_WIN // 2, D), H_WIN ** -0.5, 0.09375, ((0, 16), (1, 2)))
    shared_up = bell_draw(key_of[5], (D, SH), D ** -0.5, 0.125, ((0, 16), (1, 2)))
    shared_down = bell_draw(key_of[6], (SH, D), SH ** -0.5, 0.09375, ((0, 2), (1, 16)))
    return dict(tokens=tokens, expert_ids=expert_ids, gate_weights=gate_weights, routed_up=routed_up, routed_down=routed_down, shared_up=shared_up, shared_down=shared_down)


def reference(tokens, expert_ids, gate_weights, routed_up, routed_down, shared_up, shared_down):
    route_ids = expert_ids[:, 0].astype(jnp.int32)
    order = jnp.argsort(route_ids, stable=True).astype(jnp.int32)
    columns = jnp.arange(EXPERTS, dtype=jnp.int32)
    counts = jnp.sum((route_ids[:, None] == columns[None, :]).astype(jnp.int32), axis=0)
    starts = (jnp.cumsum(counts) - counts).astype(jnp.int32)
    bound = min(TOKENS, CAP * (TOKENS // TOK_DEV))
    padded_order = jnp.concatenate([order, jnp.zeros((bound,), jnp.int32)])
    quarter = H_WIN // (2 * N_TENSOR)

    def one_expert(routed, expert):
        rows = lax.dynamic_slice_in_dim(padded_order, starts[expert], bound)
        live = jnp.arange(bound) < counts[expert]
        chosen = tokens[rows]
        total = jnp.zeros((bound, D), jnp.float32)
        for half in range(2):
            upper = lax.dynamic_index_in_dim(routed_up, 2 * expert + half, 0, keepdims=False)
            lower = lax.dynamic_index_in_dim(routed_down, 2 * expert + half, 0, keepdims=False)
            half_total = jnp.zeros((bound, D), jnp.float32)
            for part in range(N_TENSOR):
                hidden = jax.nn.silu(jnp.dot(chosen, upper[:, part * quarter:(part + 1) * quarter], preferred_element_type=jnp.float32)).astype(jnp.bfloat16)
                half_total = half_total + jnp.dot(hidden, lower[part * quarter:(part + 1) * quarter], preferred_element_type=jnp.float32)
            piece = lax.optimization_barrier(half_total.astype(jnp.bfloat16))
            total = total + piece.astype(jnp.float32)
        total = jnp.where(live[:, None], total, jnp.zeros_like(total))
        return routed.at[rows].add(total), None

    routed, unused = lax.scan(one_expert, jnp.zeros((TOKENS, D), jnp.float32), columns)
    routed = gate_weights.astype(jnp.float32) * routed
    share = SH // N_TENSOR
    shared = jnp.zeros((TOKENS, D), jnp.float32)
    for part in range(N_TENSOR):
        hidden = jax.nn.silu(jnp.dot(tokens, shared_up[:, part * share:(part + 1) * share], preferred_element_type=jnp.float32)).astype(jnp.bfloat16)
        shared = shared + jnp.dot(hidden, shared_down[part * share:(part + 1) * share], preferred_element_type=jnp.float32)
    return (routed + shared).astype(jnp.bfloat16)
```

```python
import functools

import jax
import jax.numpy as jnp
from jax import lax
from jax.experimental import pallas as pl
from jax.experimental.pallas import tpu as pltpu
from jax.sharding import PartitionSpec as P

MESH = pl.DeviceIdType.MESH


def place_matrix(route_ids, experts, capacity):
    columns = jnp.arange(experts, dtype=jnp.int32)
    onehot = (route_ids[:, None] == columns[None, :]).astype(jnp.int32)
    before = jnp.cumsum(onehot, axis=0) - onehot
    rank_of = jnp.sum(before * onehot, axis=1)
    target = route_ids * capacity + rank_of
    slots_all = jnp.arange(experts * capacity, dtype=jnp.int32)
    return (slots_all[:, None] == target[None, :]).astype(jnp.bfloat16)


class Place:
    def __init__(self, chips):
        me = lax.axis_index("expert")
        self.chips = chips
        self.x = lax.axis_index("tensor")
        self.chip = me // 2
        self.core = me % 2
        odd = self.chip % 2
        self.pos = (1 - odd) * (self.chip // 2) + odd * (chips - 1 - self.chip // 2)

    def chip_at(self, pos):
        pos = (pos + self.chips) % self.chips
        high = pos // (self.chips // 2)
        return (1 - high) * 2 * pos + high * (2 * (self.chips - 1 - pos) + 1)

    def peer(self, chip):
        return {"expert": chip * 2 + self.core, "tensor": self.x}

    def partner(self):
        return {"expert": self.chip * 2 + 1 - self.core, "tensor": self.x}

    def across(self):
        return {"expert": self.chip * 2 + self.core, "tensor": 1 - self.x}


def greet(place):
    barrier = pltpu.get_barrier_semaphore()

    def one(step, carry):
        peer = place.peer((place.chip + step) % place.chips)
        pl.semaphore_signal(barrier, inc=1, device_id=peer, device_id_type=MESH)
        return carry

    lax.fori_loop(1, place.chips, one, 0)
    pl.semaphore_signal(barrier, inc=1, device_id=place.partner(), device_id_type=MESH)
    pl.semaphore_signal(barrier, inc=1, device_id=place.across(), device_id_type=MESH)
    pl.semaphore_wait(barrier, place.chips + 1)


def send(src, dst, sends, recvs, k, device):
    copy = pltpu.make_async_remote_copy(
        src_ref=src,
        dst_ref=dst,
        send_sem=sends.at[k],
        recv_sem=recvs.at[k],
        device_id=device,
        device_id_type=MESH,
    )
    copy.start()
    return copy


class Ring:
    def __init__(self, place, block, whole, sems):
        self.place, self.block, self.whole = place, block, whole
        self.fs, self.fr, self.bs, self.br, self.ps, self.pr, self.own = sems
        self.forward = place.chips // 2
        self.backward = place.chips - 1 - self.forward
        self.fcopies, self.bcopies, self.pcopies = [], [], []

    def slot(self, pos):
        return self.whole.at[self.place.chip_at(pos) * 2 + self.place.core]

    def hop(self, s, ahead):
        place = self.place
        pos = place.pos - s if ahead else place.pos + s
        src = self.block if s == 0 else self.slot(pos)
        if ahead and s < self.forward:
            device = place.peer(place.chip_at(place.pos + 1))
            self.fcopies.append(send(src, self.slot(pos), self.fs, self.fr, s, device))
        if not ahead and s < self.backward:
            device = place.peer(place.chip_at(place.pos - 1))
            self.bcopies.append(send(src, self.slot(pos), self.bs, self.br, s, device))
        if ahead or s > 0:
            k = s if ahead else self.forward + s
            self.pcopies.append(send(src, self.slot(pos), self.ps, self.pr, k, place.partner()))

    def start(self):
        self.hop(0, True)
        self.hop(0, False)
        self.local = pltpu.make_async_copy(self.block, self.slot(self.place.pos), self.own)
        self.local.start()

    def step(self, s):
        self.fcopies[s - 1].wait_recv()
        self.hop(s, True)
        if s <= self.backward:
            self.bcopies[s - 1].wait_recv()
            self.hop(s, False)

    def finish(self):
        self.local.wait()
        for copy in self.fcopies + self.bcopies:
            copy.wait_send()
        for copy in self.pcopies:
            copy.wait()


def ring_sems(chips):
    forward = chips // 2
    backward = max(1, chips - 1 - forward)
    dma = pltpu.SemaphoreType.DMA
    return [
        dma((forward,)),
        dma((forward,)),
        dma((backward,)),
        dma((backward,)),
        dma((chips,)),
        dma((chips,)),
        dma,
    ]


def first_kernel(chips, packed, tokens, block, arrived, other, whole, *sems):
    ring_part, (ds, dr, gs, gr, local_sem) = sems[:7], sems[7:]
    place = Place(chips)
    greet(place)
    mine = arrived.at[place.x * 2 + place.core]
    local = pltpu.make_async_copy(packed.at[place.chip], mine.at[place.chip], local_sem)
    local.start()
    dispatch = []
    for step in range(1, chips):
        chip = (place.chip + step) % chips
        dispatch.append(
            send(packed.at[chip], mine.at[place.chip], ds, dr, step, place.peer(chip))
        )
    shared = send(tokens, other, gs, gr, 0, place.across())
    ring = Ring(place, block, whole, ring_part)
    ring.start()
    local.wait()
    for copy in dispatch:
        copy.wait_recv()
    over = send(mine, mine, gs, gr, 1, place.across())
    near = send(mine, mine, gs, gr, 2, place.partner())
    last = ring.forward
    for s in range(1, last):
        ring.step(s)
    over.wait_recv()
    far = arrived.at[(1 - place.x) * 2 + place.core]
    relay = send(far, far, gs, gr, 3, place.partner())
    ring.step(last)
    ring.finish()
    for copy in dispatch:
        copy.wait_send()
    over.wait_send()
    shared.wait()
    near.wait()
    relay.wait()


def second_kernel(chips, partial, block, returned, whole, swap, cross, ours, total, *sems):
    ring_part, (rs, rr, gs, gr, local_sem) = sems[:7], sems[7:]
    place = Place(chips)
    greet(place)
    swaps = []
    for t in range(2):
        group = (1 - place.x) if t == 0 else place.x
        src = partial.at[group * 2 + 1 - place.core]
        swaps.append(send(src, swap.at[t], gs, gr, t, place.partner()))
    ring = Ring(place, block, whole, ring_part)
    ring.start()

    def add(first, second, out):
        def one(i, carry):
            out[i] = (first[i].astype(jnp.float32) + second[i].astype(jnp.float32)).astype(
                jnp.bfloat16
            )
            return carry

        lax.fori_loop(0, chips, one, 0)

    swaps[0].wait_recv()
    add(partial.at[(1 - place.x) * 2 + place.core], swap.at[0], ours)
    over = send(ours, cross, gs, gr, 2, place.across())
    swaps[1].wait_recv()
    own = partial.at[place.x * 2 + place.core]
    mid = ring.forward // 2
    for s in range(1, mid + 1):
        ring.step(s)
    over.wait_recv()

    def three(i, carry):
        total[i] = (
            own[i].astype(jnp.float32)
            + swap[1, i].astype(jnp.float32)
            + cross[i].astype(jnp.float32)
        ).astype(jnp.bfloat16)
        return carry

    lax.fori_loop(0, chips, three, 0)
    local = pltpu.make_async_copy(total.at[place.chip], returned.at[place.chip], local_sem)
    local.start()
    back = []
    for step in range(1, chips):
        chip = (place.chip + step) % chips
        back.append(send(total.at[chip], returned.at[place.chip], rs, rr, step, place.peer(chip)))
    for s in range(mid + 1, ring.forward + 1):
        ring.step(s)
    ring.finish()
    local.wait()
    for copy in back:
        copy.wait()
    over.wait_send()
    swaps[0].wait_send()
    swaps[1].wait_send()


def on_device(tokens, expert_ids, gate_weights, routed_up, routed_down, shared_up, shared_down):
    tok_rows, width = tokens.shape
    n_expert = lax.axis_size("expert")
    chips = n_expert // 2
    experts = chips
    capacity = max(2, 3 * tok_rows // (2 * experts))
    capacity = -(-capacity // 8) * 8
    rows, part = shared_up.shape
    bf16 = jnp.bfloat16
    hbm = pl.BlockSpec(memory_space=pl.ANY)
    vmem = pl.BlockSpec(memory_space=pltpu.VMEM)
    dma = pltpu.SemaphoreType.DMA
    down_rows = shared_down.T

    own_place = place_matrix(expert_ids[:, 0], experts, capacity)
    packed = jnp.dot(own_place, tokens, preferred_element_type=jnp.float32).astype(bf16)
    arrived, other, up = pl.pallas_call(
        functools.partial(first_kernel, chips),
        out_shape=[
            jax.ShapeDtypeStruct((4, chips, capacity, width), bf16),
            jax.ShapeDtypeStruct((tok_rows, width), bf16),
            jax.ShapeDtypeStruct((n_expert, rows, part), bf16),
        ],
        in_specs=[vmem] * 3,
        out_specs=[hbm] * 3,
        scratch_shapes=ring_sems(chips)
        + [dma((chips,)), dma((chips,)), dma((4,)), dma((4,)), dma],
        compiler_params=pltpu.CompilerParams(collective_id=1, has_side_effects=True),
        name="gather_up_and_dispatch",
    )(packed.reshape(experts, capacity, width), tokens, shared_up)

    flat = arrived.reshape(-1, width)
    hidden = jax.nn.silu(jnp.dot(flat, routed_up[0], preferred_element_type=jnp.float32)).astype(
        bf16
    )
    partial = jnp.dot(hidden, routed_down[0], preferred_element_type=jnp.float32).astype(bf16)
    returned, down = pl.pallas_call(
        functools.partial(second_kernel, chips),
        out_shape=[
            jax.ShapeDtypeStruct((chips, capacity, width), bf16),
            jax.ShapeDtypeStruct((n_expert, rows, part), bf16),
        ],
        in_specs=[vmem] * 2,
        out_specs=[hbm] * 2,
        scratch_shapes=[
            pltpu.VMEM((2, chips, capacity, width), bf16),
            pltpu.VMEM((chips, capacity, width), bf16),
            pltpu.VMEM((chips, capacity, width), bf16),
            pltpu.VMEM((chips, capacity, width), bf16),
        ]
        + ring_sems(chips)
        + [dma((chips,)), dma((chips,)), dma((3,)), dma((3,)), dma],
        compiler_params=pltpu.CompilerParams(
            collective_id=2, has_side_effects=True, vmem_limit_bytes=60 * 1024 * 1024
        ),
        name="gather_down_and_return",
    )(partial.reshape(4, chips, capacity, width), down_rows)

    both = jnp.concatenate([tokens, other], axis=0)
    shared_acc = jnp.dot(both, up.reshape(n_expert * rows, part), preferred_element_type=jnp.float32)
    shared_hidden = jax.nn.silu(shared_acc).astype(bf16)
    shared_part = lax.dot_general(
        shared_hidden,
        down.reshape(n_expert * rows, part),
        (((1,), (1,)), ((), ())),
        preferred_element_type=jnp.float32,
    )
    theirs = lax.ppermute(shared_part[tok_rows:].astype(bf16), "tensor", [(0, 1), (1, 0)])
    routed = jnp.einsum(
        "st,sd->td",
        own_place,
        returned.reshape(experts * capacity, width),
        preferred_element_type=jnp.float32,
    )
    routed = gate_weights.astype(jnp.float32) * routed
    return (routed + shared_part[:tok_rows] + theirs.astype(jnp.float32)).astype(bf16)


def solution(mesh):
    placed = (
        P(("expert", "tensor"), None),
        P(("expert", "tensor"), None),
        P(("expert", "tensor"), None),
        P("expert", None, "tensor"),
        P("expert", "tensor", None),
        P("expert", "tensor"),
        P("tensor", "expert"),
    )
    return jax.shard_map(
        on_device,
        mesh=mesh,
        in_specs=placed,
        out_specs=P(("expert", "tensor"), None),
        check_vma=False,
    )
```

```python
import functools

import jax
import jax.numpy as jnp
from jax import lax
from jax.experimental import pallas as pl
from jax.experimental.pallas import tpu as pltpu
from jax.sharding import PartitionSpec as P

MESH = pl.DeviceIdType.MESH


def place_matrix(route_ids, experts, capacity):
    columns = jnp.arange(experts, dtype=jnp.int32)
    onehot = (route_ids[:, None] == columns[None, :]).astype(jnp.int32)
    before = jnp.cumsum(onehot, axis=0) - onehot
    rank_of = jnp.sum(before * onehot, axis=1)
    target = route_ids * capacity + rank_of
    slots_all = jnp.arange(experts * capacity, dtype=jnp.int32)
    return (slots_all[:, None] == target[None, :]).astype(jnp.bfloat16)


class Place:
    def __init__(self, chips):
        me = lax.axis_index("expert")
        self.chips = chips
        self.x = lax.axis_index("tensor")
        self.chip = me // 2
        self.core = me % 2
        odd = self.chip % 2
        self.pos = (1 - odd) * (self.chip // 2) + odd * (chips - 1 - self.chip // 2)

    def chip_at(self, pos):
        pos = (pos + self.chips) % self.chips
        high = pos // (self.chips // 2)
        return (1 - high) * 2 * pos + high * (2 * (self.chips - 1 - pos) + 1)

    def peer(self, chip):
        return {"expert": chip * 2 + self.core, "tensor": self.x}

    def partner(self):
        return {"expert": self.chip * 2 + 1 - self.core, "tensor": self.x}

    def across(self):
        return {"expert": self.chip * 2 + self.core, "tensor": 1 - self.x}


def greet(place):
    barrier = pltpu.get_barrier_semaphore()

    def one(step, carry):
        peer = place.peer((place.chip + step) % place.chips)
        pl.semaphore_signal(barrier, inc=1, device_id=peer, device_id_type=MESH)
        return carry

    lax.fori_loop(1, place.chips, one, 0)
    pl.semaphore_signal(barrier, inc=1, device_id=place.partner(), device_id_type=MESH)
    pl.semaphore_signal(barrier, inc=1, device_id=place.across(), device_id_type=MESH)
    pl.semaphore_wait(barrier, place.chips + 1)


def send(src, dst, sends, recvs, k, device):
    copy = pltpu.make_async_remote_copy(
        src_ref=src,
        dst_ref=dst,
        send_sem=sends.at[k],
        recv_sem=recvs.at[k],
        device_id=device,
        device_id_type=MESH,
    )
    copy.start()
    return copy


class Ring:
    def __init__(self, place, block, whole, sems, piece, pieces):
        rows = block.shape[0] // pieces
        self.rows = pl.ds(piece * rows, rows)
        self.place, self.block, self.whole = place, block.at[self.rows], whole
        self.fs, self.fr, self.bs, self.br, self.ps, self.pr, self.own = sems
        longer = place.chips // 2
        self.forward = longer if piece == 0 else place.chips - 1 - longer
        self.backward = place.chips - 1 - self.forward
        self.fcopies, self.bcopies, self.pcopies = [], [], []

    def slot(self, pos):
        return self.whole.at[self.place.chip_at(pos) * 2 + self.place.core, self.rows]

    def hop(self, s, ahead):
        place = self.place
        pos = place.pos - s if ahead else place.pos + s
        src = self.block if s == 0 else self.slot(pos)
        if ahead and s < self.forward:
            device = place.peer(place.chip_at(place.pos + 1))
            self.fcopies.append(send(src, self.slot(pos), self.fs, self.fr, s, device))
        if not ahead and s < self.backward:
            device = place.peer(place.chip_at(place.pos - 1))
            self.bcopies.append(send(src, self.slot(pos), self.bs, self.br, s, device))
        if ahead or s > 0:
            k = s if ahead else self.forward + s
            self.pcopies.append(send(src, self.slot(pos), self.ps, self.pr, k, place.partner()))

    def start(self):
        self.hop(0, True)
        self.hop(0, False)
        self.local = pltpu.make_async_copy(self.block, self.slot(self.place.pos), self.own)
        self.local.start()

    def step(self, s, ahead):
        if s <= (self.forward if ahead else self.backward):
            (self.fcopies if ahead else self.bcopies)[s - 1].wait_recv()
            self.hop(s, ahead)

    def finish(self):
        self.local.wait()
        for copy in self.fcopies + self.bcopies:
            copy.wait_send()
        for copy in self.pcopies:
            copy.wait()


class Rings:
    def __init__(self, place, block, whole, sems):
        pieces = len(sems) // RING_SEMS
        self.steps = place.chips // 2
        self.rings = [
            Ring(place, block, whole, sems[p * RING_SEMS : (p + 1) * RING_SEMS], p, pieces)
            for p in range(pieces)
        ]

    def start(self):
        for ring in self.rings:
            ring.start()

    def step(self, s):
        for p in range(len(self.rings)):
            self.rings[p].step(s, True)
            self.rings[-1 - p].step(s, False)

    def finish(self):
        for ring in self.rings:
            ring.finish()


RING_SEMS = 7


def pieces_of(rows):
    return 2 if rows % 16 == 0 else 1


def ring_sems(chips, pieces):
    dma = pltpu.SemaphoreType.DMA
    return ([dma((chips // 2,))] * 4 + [dma((chips,)), dma((chips,)), dma]) * pieces


def first_kernel(chips, packed, tokens, block, arrived, other, whole, *sems):
    ring_part, (ds, dr, gs, gr, local_sem) = sems[:-5], sems[-5:]
    place = Place(chips)
    greet(place)
    mine = arrived.at[place.x * 2 + place.core]
    local = pltpu.make_async_copy(packed.at[place.chip], mine.at[place.chip], local_sem)
    local.start()
    dispatch = []
    for step in range(1, chips):
        chip = (place.chip + step) % chips
        dispatch.append(
            send(packed.at[chip], mine.at[place.chip], ds, dr, step, place.peer(chip))
        )
    shared = send(tokens, other, gs, gr, 0, place.across())
    ring = Rings(place, block, whole, ring_part)
    ring.start()
    local.wait()
    for copy in dispatch:
        copy.wait_recv()
    over = send(mine, mine, gs, gr, 1, place.across())
    near = send(mine, mine, gs, gr, 2, place.partner())
    last = ring.steps
    for s in range(1, last):
        ring.step(s)
    over.wait_recv()
    far = arrived.at[(1 - place.x) * 2 + place.core]
    relay = send(far, far, gs, gr, 3, place.partner())
    ring.step(last)
    ring.finish()
    for copy in dispatch:
        copy.wait_send()
    over.wait_send()
    shared.wait()
    near.wait()
    relay.wait()


def second_kernel(chips, partial, block, returned, whole, swap, cross, ours, total, *sems):
    ring_part, (rs, rr, gs, gr, local_sem) = sems[:-5], sems[-5:]
    place = Place(chips)
    greet(place)
    swaps = []
    for t in range(2):
        group = (1 - place.x) if t == 0 else place.x
        src = partial.at[group * 2 + 1 - place.core]
        swaps.append(send(src, swap.at[t], gs, gr, t, place.partner()))
    ring = Rings(place, block, whole, ring_part)
    ring.start()

    def add(first, second, out):
        def one(i, carry):
            out[i] = (first[i].astype(jnp.float32) + second[i].astype(jnp.float32)).astype(
                jnp.bfloat16
            )
            return carry

        lax.fori_loop(0, chips, one, 0)

    swaps[0].wait_recv()
    add(partial.at[(1 - place.x) * 2 + place.core], swap.at[0], ours)
    over = send(ours, cross, gs, gr, 2, place.across())
    swaps[1].wait_recv()
    own = partial.at[place.x * 2 + place.core]
    mid = ring.steps // 2
    for s in range(1, mid + 1):
        ring.step(s)
    over.wait_recv()

    def three(i, carry):
        total[i] = (
            own[i].astype(jnp.float32)
            + swap[1, i].astype(jnp.float32)
            + cross[i].astype(jnp.float32)
        ).astype(jnp.bfloat16)
        return carry

    lax.fori_loop(0, chips, three, 0)
    local = pltpu.make_async_copy(total.at[place.chip], returned.at[place.chip], local_sem)
    local.start()
    back = []
    for step in range(1, chips):
        chip = (place.chip + step) % chips
        back.append(send(total.at[chip], returned.at[place.chip], rs, rr, step, place.peer(chip)))
    for s in range(mid + 1, ring.steps + 1):
        ring.step(s)
    ring.finish()
    local.wait()
    for copy in back:
        copy.wait()
    over.wait_send()
    swaps[0].wait_send()
    swaps[1].wait_send()


def on_device(tokens, expert_ids, gate_weights, routed_up, routed_down, shared_up, shared_down):
    tok_rows, width = tokens.shape
    n_expert = lax.axis_size("expert")
    chips = n_expert // 2
    experts = chips
    capacity = max(2, 3 * tok_rows // (2 * experts))
    capacity = -(-capacity // 8) * 8
    rows, part = shared_up.shape
    bf16 = jnp.bfloat16
    hbm = pl.BlockSpec(memory_space=pl.ANY)
    vmem = pl.BlockSpec(memory_space=pltpu.VMEM)
    dma = pltpu.SemaphoreType.DMA
    down_rows = shared_down.T

    own_place = place_matrix(expert_ids[:, 0], experts, capacity)
    packed = jnp.dot(own_place, tokens, preferred_element_type=jnp.float32).astype(bf16)
    arrived, other, up = pl.pallas_call(
        functools.partial(first_kernel, chips),
        out_shape=[
            jax.ShapeDtypeStruct((4, chips, capacity, width), bf16),
            jax.ShapeDtypeStruct((tok_rows, width), bf16),
            jax.ShapeDtypeStruct((n_expert, rows, part), bf16),
        ],
        in_specs=[vmem] * 3,
        out_specs=[hbm] * 3,
        scratch_shapes=ring_sems(chips, pieces_of(rows))
        + [dma((chips,)), dma((chips,)), dma((4,)), dma((4,)), dma],
        compiler_params=pltpu.CompilerParams(collective_id=1, has_side_effects=True),
        name="gather_up_and_dispatch",
    )(packed.reshape(experts, capacity, width), tokens, shared_up)

    flat = arrived.reshape(-1, width)
    hidden = jax.nn.silu(jnp.dot(flat, routed_up[0], preferred_element_type=jnp.float32)).astype(
        bf16
    )
    partial = jnp.dot(hidden, routed_down[0], preferred_element_type=jnp.float32).astype(bf16)
    returned, down = pl.pallas_call(
        functools.partial(second_kernel, chips),
        out_shape=[
            jax.ShapeDtypeStruct((chips, capacity, width), bf16),
            jax.ShapeDtypeStruct((n_expert, rows, part), bf16),
        ],
        in_specs=[vmem] * 2,
        out_specs=[hbm] * 2,
        scratch_shapes=[
            pltpu.VMEM((2, chips, capacity, width), bf16),
            pltpu.VMEM((chips, capacity, width), bf16),
            pltpu.VMEM((chips, capacity, width), bf16),
            pltpu.VMEM((chips, capacity, width), bf16),
        ]
        + ring_sems(chips, pieces_of(rows))
        + [dma((chips,)), dma((chips,)), dma((3,)), dma((3,)), dma],
        compiler_params=pltpu.CompilerParams(
            collective_id=2, has_side_effects=True, vmem_limit_bytes=60 * 1024 * 1024
        ),
        name="gather_down_and_return",
    )(partial.reshape(4, chips, capacity, width), down_rows)

    both = jnp.concatenate([tokens, other], axis=0)
    shared_acc = jnp.dot(both, up.reshape(n_expert * rows, part), preferred_element_type=jnp.float32)
    shared_hidden = jax.nn.silu(shared_acc).astype(bf16)
    shared_part = lax.dot_general(
        shared_hidden,
        down.reshape(n_expert * rows, part),
        (((1,), (1,)), ((), ())),
        preferred_element_type=jnp.float32,
    )
    theirs = lax.ppermute(shared_part[tok_rows:].astype(bf16), "tensor", [(0, 1), (1, 0)])
    routed = jnp.einsum(
        "st,sd->td",
        own_place,
        returned.reshape(experts * capacity, width),
        preferred_element_type=jnp.float32,
    )
    routed = gate_weights.astype(jnp.float32) * routed
    return (routed + shared_part[:tok_rows] + theirs.astype(jnp.float32)).astype(bf16)


def solution(mesh):
    placed = (
        P(("expert", "tensor"), None),
        P(("expert", "tensor"), None),
        P(("expert", "tensor"), None),
        P("expert", None, "tensor"),
        P("expert", "tensor", None),
        P("expert", "tensor"),
        P("tensor", "expert"),
    )
    return jax.shard_map(
        on_device,
        mesh=mesh,
        in_specs=placed,
        out_specs=P(("expert", "tensor"), None),
        check_vma=False,
    )
```
